512 devices in a mesh: fsdp: 16 (over y, x), tp: 16 (over z), shift: 2 (over core).
Axes of the slice: x: 4, y: 4, z: 16, core: 2. Of those that a mesh axis runs over, the one named last changes fastest.
Arguments:
- w_query: float32 [10240, 5120], P(('shift', 'fsdp'), 'tp'), parts along dimension 0, may hold values from -0.125 to 0.125
- avg_query: float32 [10240, 5120], P(('shift', 'fsdp'), 'tp'), parts along dimension 0, may hold values from -0.078125 to 0.078125
- w_key: float32 [10240, 5120], P(('shift', 'fsdp'), 'tp'), parts along dimension 0, may hold values from -0.125 to 0.125
- avg_key: float32 [10240, 5120], P(('shift', 'fsdp'), 'tp'), parts along dimension 0, may hold values from -0.078125 to 0.078125
- w_value: float32 [10240, 5120], P(('shift', 'fsdp'), 'tp'), parts along dimension 0, may hold values from -0.125 to 0.125
- avg_value: float32 [10240, 5120], P(('shift', 'fsdp'), 'tp'), parts along dimension 0, may hold values from -0.078125 to 0.078125
- norm_train: float32 [10240], P(('shift', 'fsdp', 'tp')), parts along dimension 0, may hold values from 0.25 to 1.75
- norm_step: float32 [10240], P(('shift', 'fsdp', 'tp')), parts along dimension 0, may hold values from -0.3 to 0.3
Outputs:
- ready_query: bfloat16 [10240, 5120], P('shift', 'tp'), parts along dimension 0
- ready_key: bfloat16 [10240, 5120], P('shift', 'tp'), parts along dimension 0
- ready_value: bfloat16 [10240, 5120], P('shift', 'tp'), parts along dimension 0
- scale_query: float32 [10240], P(('shift', 'tp')), parts along dimension 0
- scale_key: float32 [10240], P(('shift', 'tp')), parts along dimension 0
- scale_value: float32 [10240], P(('shift', 'tp')), parts along dimension 0
- serve_norm: bfloat16 [10240], P('shift'), parts along dimension 0
- latest_query: float32 [10240, 5120], P(('shift', 'fsdp'), 'tp'), parts along dimension 0
- latest_key: float32 [10240, 5120], P(('shift', 'fsdp'), 'tp'), parts along dimension 0
- latest_value: float32 [10240, 5120], P(('shift', 'fsdp'), 'tp'), parts along dimension 0
The draws below stay inside these ranges and needn't reach their ends.
There are 2 independent parts, one for each index of `shift`. The reference program is written for one: setup_inputs(seed, part) draws one part's arguments, and reference() takes and returns one part's arrays. A program takes and returns all parts, laid end to end along the dimension named above; each array names one. Nothing has to cross between parts.
All inputs are finite; a program needn't handle non-finite values. Where the reference program divides by a largest or mean magnitude, that divisor is 1e-20 or more.
Results may differ from the reference program's by a relative error of at most 0.001.
Values may be sent and summed in bfloat16 or wider, within the bound.
No kernel may reach another device: no remote copies, remote signals or barrier semaphores. Data moves between devices by JAX's collectives and lax.ppermute only.
A program may use at most 128 MiB of HBM per device.

```python
import jax
import jax.numpy as jnp

D_MODEL = 5120
Q_DIM = 5120
KV_DIM = 5120


def raised(drawn, rng, source, target, blocks, factor):
    owner, partner = [(jnp.arange(drawn.shape[dim]) // (drawn.shape[dim] // blocks)).reshape([-1 if axis == dim else 1 for axis in range(drawn.ndim)]) for dim in (source, target)]
    chosen = jax.random.permutation(rng, blocks)[partner]
    strong = (owner == chosen) | (owner == (partner + blocks // 2) % blocks)
    return jnp.where(strong, factor * drawn, drawn)


def steps_of(rng, shape, pieces, low, top_value):
    gain = 1.0
    for dim, blocks in pieces:
        heights = jax.random.uniform(jax.random.fold_in(jax.random.fold_in(rng, 6), dim), (blocks,), jnp.float32, low / len(pieces), top_value / len(pieces))
        gain = gain * jnp.repeat(jnp.exp(heights), shape[dim] // blocks).reshape((-1,) + (1,) * (len(shape) - 1 - dim))
    return gain


def normal_values(own_key, shape, scale, most, cuts=(), dtype=jnp.bfloat16):
    loudness = steps_of(own_key, shape, cuts, -0.22, 0.18) if cuts else 1.0
    entries = jax.random.normal(own_key, shape, jnp.float32) * scale * loudness
    return jnp.minimum(jnp.maximum(entries, -most), most).astype(dtype)


def gaussian_with(stream_key, extent, spread, reach, split, heavy, dtype=jnp.bfloat16):
    values = spread * jax.random.normal(stream_key, extent, jnp.float32)
    if split:
        values = values * steps_of(stream_key, extent, split, -0.22, 0.18)
    return jnp.clip(raised(values, jax.random.fold_in(stream_key, 3), *heavy), -reach, reach).astype(dtype)


def setup_inputs(seed: int = 0, part: int = 0) -> dict:
    splits = jax.random.split(jax.random.key(seed), 9)
    own_keys = jax.random.split(jax.random.fold_in(splits[8], part), 9)
    w_query = gaussian_with(own_keys[0], (D_MODEL, Q_DIM), D_MODEL ** -0.5, 0.125, ((0, 16), (1, 16)), (0, 1, 16, 2.0), jnp.float32)
    avg_query = normal_values(own_keys[1], (D_MODEL, Q_DIM), D_MODEL ** -0.5, 0.078125, ((0, 16), (1, 16)), jnp.float32)
    w_key = gaussian_with(own_keys[2], (D_MODEL, KV_DIM), D_MODEL ** -0.5, 0.125, ((0, 16), (1, 16)), (0, 1, 16, 2.0), jnp.float32)
    avg_key = normal_values(own_keys[3], (D_MODEL, KV_DIM), D_MODEL ** -0.5, 0.078125, ((0, 16), (1, 16)), jnp.float32)
    w_value = gaussian_with(own_keys[4], (D_MODEL, KV_DIM), D_MODEL ** -0.5, 0.125, ((0, 16), (1, 16)), (0, 1, 16, 2.0), jnp.float32)
    avg_value = normal_values(own_keys[5], (D_MODEL, KV_DIM), D_MODEL ** -0.5, 0.078125, ((0, 16), (1, 16)), jnp.float32)
    norm_train = jnp.clip(1.0 + 0.15 * jax.random.normal(own_keys[6], (D_MODEL,), jnp.float32), 0.25, 1.75)
    norm_step = jnp.clip(jax.random.uniform(own_keys[7], (D_MODEL,), jnp.float32, -0.3, 0.3) * steps_of(own_keys[7], (D_MODEL,), ((0, 256),), -0.4, 0.0), -0.3, 0.3)
    return {"w_query": w_query, "avg_query": avg_query, "w_key": w_key, "avg_key": avg_key, "w_value": w_value, "avg_value": avg_value, "norm_train": norm_train, "norm_step": norm_step}


keep_rate = 0.7


def reference(w_query, avg_query, w_key, avg_key, w_value, avg_value, norm_train, norm_step):
    latest_query = keep_rate * avg_query + (1.0 - keep_rate) * w_query
    latest_key = keep_rate * avg_key + (1.0 - keep_rate) * w_key
    latest_value = keep_rate * avg_value + (1.0 - keep_rate) * w_value
    scale_query = jnp.sum(jnp.abs(latest_query), axis=0) / D_MODEL
    ready_query = (latest_query / scale_query).astype(jnp.bfloat16)
    scale_key = jnp.sum(jnp.abs(latest_key), axis=0) / D_MODEL
    ready_key = (latest_key / scale_key).astype(jnp.bfloat16)
    scale_value = jnp.sum(jnp.abs(latest_value), axis=0) / D_MODEL
    ready_value = (latest_value / scale_value).astype(jnp.bfloat16)
    serve_norm = (norm_train + norm_step).astype(jnp.bfloat16)
    return ready_query, ready_key, ready_value, scale_query, scale_key, scale_value, serve_norm, latest_query, latest_key, latest_value
```

```python
import functools

import jax
import jax.numpy as jnp
from jax import lax
from jax.experimental import pallas as pl
from jax.experimental.pallas import tpu as pltpu
from jax.sharding import Mesh
from jax.sharding import PartitionSpec as P


D_MODEL = 5120
FSDP = ("fsdp_0", "fsdp_1")
SHIFT_FSDP = ("shift", "fsdp_0", "fsdp_1")
SHIFT_FSDP_TP = ("shift", "fsdp_0", "fsdp_1", "tp")

keep_rate = 0.7

ROWS = 320
COLS = 320
NODES = 16
WIDTH = (256, 256, 224, 224)
START = (0, 256, 512, 736)
NEAR = ((0, 1), (1, 0), (2, 3), (3, 2))
FAR = ((1, 2), (2, 1), (3, 0), (0, 3))
CLASSES = (("fsdp_1", NEAR, 0), ("fsdp_1", FAR, 1), ("fsdp_0", NEAR, 0), ("fsdp_0", FAR, 1))
EARLY = (1, 2, 3)
ORDER = tuple(tuple((colour + step + 1) % 4 for step in range(4)) for colour in range(4))


def lines(colour):
    return WIDTH[colour] * 5 // 2


def average_kernel(wq, aq, wk, ak, wv, av, nt, ns, lq, lk, lv, sent, flat):
    flat[...] = jnp.zeros_like(flat)
    for m, (w, a, out) in enumerate(((wq, aq, lq), (wk, ak, lk), (wv, av, lv))):
        latest = keep_rate * a[...] + (1.0 - keep_rate) * w[...]
        out[...] = latest
        flat[m : m + 1, :COLS] = jnp.sum(jnp.abs(latest), axis=0, keepdims=True)
    flat[3:4, :20] = nt[...] + ns[...]
    row = lax.broadcasted_iota(jnp.int32, (8, 128), 0)
    lane = lax.broadcasted_iota(jnp.int32, (8, 128), 1)
    first, second, third = flat[:, :128], flat[:, 128:256], flat[:, 256:384]
    turned = pltpu.roll(third, 64, 1)
    packed = jnp.where(row < 4, first, pltpu.roll(second, 4, 0))
    packed = jnp.where((row == 3) & (lane >= 64), pltpu.roll(turned, 1, 0), packed)
    packed = jnp.where(
        row == 7,
        jnp.where(lane < 64, pltpu.roll(third, 7, 0), pltpu.roll(turned, 6, 0)),
        packed,
    )
    for node in range(NODES):
        sent[node] = packed


def pack_kernel(got, lq, lk, lv, m0, m1, m2, m3, sq, sk, sv, norm, wide):
    odd = lax.rem(lax.axis_index("fsdp_1"), 2) == 1
    total = got[0]
    for node in range(1, NODES):
        total = total + got[node]
    scale = total / D_MODEL
    turned = pltpu.roll(scale, 64, 1)
    tails = (scale[7:8], turned[7:8], turned[3:4])
    for m, (latest, out) in enumerate(((lq, sq), (lk, sk), (lv, sv))):
        parts = (scale[m : m + 1], scale[4 + m : 5 + m], tails[m][:, :64])
        for k, part in enumerate(parts):
            here = slice(128 * k, 128 * k + part.shape[1])
            out[here] = part[0]
            ready = latest[:, here] / part
            wide[COLS * m + here.start : COLS * m + here.stop, :ROWS] = ready.T
    norm[...] = jnp.zeros_like(norm)
    for node in range(NODES):
        norm[node : node + 1, :] = got[node, 3:4, :].astype(jnp.bfloat16)
    low = lax.broadcasted_iota(jnp.int32, (128, 128), 1) < 64
    for colour, out in enumerate((m0, m1, m2, m3)):
        width, start = WIDTH[colour], START[colour]
        half = width // 2
        mine = slice(start, start + width)

        @pl.when(jnp.logical_not(odd))
        def _(out=out, mine=mine, width=width, half=half):
            out[:width] = wide[mine, :128].astype(jnp.bfloat16)
            out[width : 2 * width] = wide[mine, 128:256].astype(jnp.bfloat16)
            rest = wide[mine, 256:384]
            both = jnp.where(low[:half], rest[:half], pltpu.roll(rest[half:], 64, 1))
            out[2 * width :] = both.astype(jnp.bfloat16)

        @pl.when(odd)
        def _(out=out, mine=mine, width=width, half=half):
            one = pltpu.roll(wide[mine, :128], 64, 1)
            two = pltpu.roll(wide[mine, 128:256], 64, 1)
            three = pltpu.roll(wide[mine, 256:384], 64, 1)
            cut = lax.broadcasted_iota(jnp.int32, (width, 128), 1) < 64
            out[:width] = jnp.where(cut, one, two).astype(jnp.bfloat16)
            out[width : 2 * width] = jnp.where(cut, two, three).astype(jnp.bfloat16)
            both = jnp.where(low[:half], pltpu.roll(one[half:], 64, 1), one[:half])
            out[2 * width :] = both.astype(jnp.bfloat16)


def place_of(colour, j):
    flips = {"fsdp_0": 0, "fsdp_1": 0}
    for step, cls in enumerate(ORDER[colour]):
        axis, _, bit = CLASSES[cls]
        if j >> step & 1:
            flips[axis] |= 1 << bit
    at = []
    for axis in FSDP:
        i = lax.axis_index(axis)
        gray = (i ^ (i >> 1)) ^ flips[axis]
        at.append(gray ^ (gray >> 1))
    return at[0] * 4 + at[1]


SEGMENTS = []
for _colour in range(4):
    _cut = []
    for _m in range(3):
        _lo = max(START[_colour], COLS * _m)
        _hi = min(START[_colour] + WIDTH[_colour], COLS * (_m + 1))
        if _lo < _hi:
            _cut.append((_m, _lo - COLS * _m, _lo - START[_colour], _hi - _lo))
    SEGMENTS.append(tuple(_cut))


def unpack_kernel(jobs, touched, given, *refs):
    outs = dict(zip(touched, refs[given : given + len(touched)]))
    scratch = refs[given + len(touched) :]
    started = []
    for n, (colour, pairs, halves) in enumerate(jobs):
        block, in_sem = scratch[4 * n], scratch[4 * n + 2]
        size = lines(colour)
        places = []
        for i, pair in enumerate(pairs):
            for j in pair:
                place = place_of(colour, j)
                slot = 2 * i + (place & 1)
                src = refs[halves[j // 8]].at[pl.ds((j % 8) * size, size)]
                pltpu.make_async_copy(src, block.at[slot], in_sem.at[slot]).start()
            places.append(place >> 1)
        started.append(places)
    going = []
    for n, (colour, _, halves) in enumerate(jobs):
        block, out, in_sem, out_sem = scratch[4 * n : 4 * n + 4]
        size, width = lines(colour), WIDTH[colour]
        half = width // 2
        low = lax.broadcasted_iota(jnp.int32, (half, 128), 1) < 64
        for i, place in enumerate(started[n]):
            for slot in (2 * i, 2 * i + 1):
                src = refs[min(halves.values())].at[pl.ds(0, size)]
                pltpu.make_async_copy(src, block.at[slot], in_sem.at[slot]).wait()
            even, odd = block.at[2 * i], block.at[2 * i + 1]
            lane = 640 * i
            out[:, lane : lane + 128] = even[:width]
            out[:, lane + 128 : lane + 256] = even[width : 2 * width]
            out[:, lane + 384 : lane + 512] = odd[:width]
            out[:, lane + 512 : lane + 640] = odd[width : 2 * width]
            e = even[2 * width :].astype(jnp.float32)
            o = odd[2 * width :].astype(jnp.float32)
            out[:half, lane + 256 : lane + 384] = jnp.where(low, e, o).astype(jnp.bfloat16)
            out[half:, lane + 256 : lane + 384] = pltpu.roll(
                jnp.where(low, o, e), 64, 1
            ).astype(jnp.bfloat16)
            there = pl.ds(pl.multiple_of(place * 640, 128), 640)
            for k, (m, to, at, many) in enumerate(SEGMENTS[colour]):
                copy = pltpu.make_async_copy(
                    out.at[pl.ds(at, many), pl.ds(lane, 640)],
                    outs[m].at[pl.ds(to, many), there],
                    out_sem.at[k, i],
                )
                copy.start()
                going.append(copy)
    for copy in going:
        copy.wait()


def unpacked(work, ready):
    values, jobs, scratch, size = [], [], [], 0
    for colour, nodes, halves in work:
        pairs = pairs_of(colour, nodes)
        at = {}
        for half, value in halves.items():
            at[half] = len(values)
            values.append(value)
        jobs.append((colour, pairs, at))
        scratch += [
            pltpu.VMEM((2 * len(pairs), lines(colour), 128), BF16),
            pltpu.VMEM((WIDTH[colour], 640 * len(pairs)), BF16),
            pltpu.SemaphoreType.DMA((2 * len(pairs),)),
            pltpu.SemaphoreType.DMA((2, len(pairs))),
        ]
        size += 4 * lines(colour) * 128 * len(pairs)
    touched = sorted({m for colour, _, _ in work for m, _, _, _ in SEGMENTS[colour]})
    begun = [m for m in touched if m in ready]
    given = len(values) + len(begun)
    result = pl.pallas_call(
        functools.partial(unpack_kernel, jobs, touched, given),
        out_shape=tuple(jax.ShapeDtypeStruct((COLS, D_MODEL), BF16) for _ in touched),
        in_specs=[ANY] * given,
        out_specs=[ANY] * len(touched),
        input_output_aliases={len(values) + i: touched.index(m) for i, m in enumerate(begun)},
        scratch_shapes=scratch,
        cost_estimate=pl.CostEstimate(flops=size, bytes_accessed=4 * size, transcendentals=0),
    )(*values, *(ready[m] for m in begun))
    ready.update(zip(touched, result))


def pairs_of(colour, nodes):
    flip = 1 << ORDER[colour].index(0)
    return tuple((j, j | flip) for j in nodes if not j & flip and j | flip in nodes)


VMEM = pl.BlockSpec(memory_space=pltpu.VMEM)
ANY = pl.BlockSpec(memory_space=pl.ANY)
F32 = jnp.float32
BF16 = jnp.bfloat16


def shards(w_query, avg_query, w_key, avg_key, w_value, avg_value, norm_train, norm_step):
    square = jax.ShapeDtypeStruct((ROWS, COLS), F32)
    lq, lk, lv, sums = pl.pallas_call(
        average_kernel,
        out_shape=(square,) * 3 + (jax.ShapeDtypeStruct((NODES, 8, 128), F32),),
        in_specs=[VMEM] * 8,
        out_specs=[VMEM] * 4,
        scratch_shapes=[pltpu.VMEM((8, 384), F32)],
    )(
        w_query,
        avg_query,
        w_key,
        avg_key,
        w_value,
        avg_value,
        norm_train.reshape(1, 20),
        norm_step.reshape(1, 20),
    )
    got = lax.all_to_all(sums, FSDP, 0, 0)
    row = jax.ShapeDtypeStruct((COLS,), F32)
    *own, sq, sk, sv, norm = pl.pallas_call(
        pack_kernel,
        out_shape=tuple(pltpu.VMEM((lines(c), 128), BF16) for c in range(4))
        + (row,) * 3
        + (jax.ShapeDtypeStruct((NODES, 128), BF16),),
        in_specs=[VMEM] * 4,
        out_specs=[VMEM] * 8,
        scratch_shapes=[pltpu.VMEM((3 * COLS, 384), F32)],
    )(got, lq, lk, lv)

    def exchanged(value, colour, step):
        axis, pairs, _ = CLASSES[ORDER[colour][step]]
        return lax.ppermute(value, axis, pairs)

    held = list(own)
    ready = {}
    for step in range(4):
        came = [exchanged(held[c], c, step) for c in range(4)]
        if step < 3:
            for c in range(4):
                both = jnp.concatenate([held[c], came[c]], axis=0)
                held[c] = lax.optimization_barrier(both)
    wide = jnp.broadcast_to(norm[None], (NODES, NODES, 128))
    norms = lax.all_to_all(wide, "tp", 0, 0)
    unpacked([(c, range(8), {0: held[c]}) for c in EARLY], ready)
    for c in range(4):
        if c in EARLY:
            unpacked([(c, range(8, 16), {1: came[c]})], ready)
        else:
            unpacked([(c, range(16), {0: held[c], 1: came[c]})], ready)
    serve_norm = norms[:, :, :20].transpose(1, 0, 2).reshape(D_MODEL)

    return (
        *(ready[m].T for m in range(3)),
        sq,
        sk,
        sv,
        serve_norm,
        lq,
        lk,
        lv,
    )


def solution(mesh):
    split = Mesh(
        mesh.devices.reshape(4, 4, mesh.shape["tp"], mesh.shape["shift"]),
        ("fsdp_0", "fsdp_1", "tp", "shift"),
    )
    in_specs = (P(SHIFT_FSDP, "tp"),) * 6 + (P(SHIFT_FSDP_TP),) * 2
    out_specs = (
        (P("shift", "tp"),) * 3
        + (P(("shift", "tp")),) * 3
        + (P("shift"),)
        + (P(SHIFT_FSDP, "tp"),) * 3
    )
    return jax.shard_map(
        shards, mesh=split, in_specs=in_specs, out_specs=out_specs, check_vma=False
    )
```
